32 devices in a mesh: row: 4 (over y, core), col: 8 (over z, x).
Axes of the slice: x: 2, y: 2, z: 4, core: 2. Of those that a mesh axis runs over, the one named last changes fastest.
Arguments:
- master: float32 [8, 1792, 3584], P('col', 'row'), may hold values from -6 to 6
- grad: bfloat16 [8, 1792, 3584], P('col', 'row'), may hold values from -6 to 6
- first_moment: float32 [8, 1792, 3584], P('col', 'row'), may hold values from -6 to 6
- second_moment: float32 [8, 1792, 3584], P('col', 'row'), may hold values from 0.05 to 2
- basis: bfloat16 [8, 1792, 3584], P('col', 'row'), may hold values from -0.0625 to 0.0625
Outputs:
- new_master: float32 [8, 1792, 3584], P('col', 'row')
- new_weight: bfloat16 [8, 1792, 3584], P('col', 'row')
- new_first: float32 [8, 1792, 3584], P('col', 'row')
- new_second: float32 [8, 1792, 3584], P('col', 'row')
The draws below stay inside these ranges and needn't reach their ends.
All inputs are finite; a program needn't handle non-finite values.
Results may differ from the reference program's by a relative error of at most 0.0065.
Values may be sent and summed in bfloat16 or wider, within the bound.
A program may use at most 192 MiB of HBM per device.

```python
import math
import jax
import jax.numpy as jnp
from jax import lax

D = 7168
N_ROW = 4
N_COL = 8


def shard_levels(own_key, extent, cuts, low, top_value):
    loudness = 1.0
    for dim, blocks in cuts:
        heights = jax.random.uniform(jax.random.fold_in(jax.random.fold_in(own_key, 6), dim), (blocks,), jnp.float32, low / len(cuts), top_value / len(cuts))
        loudness = loudness * jnp.repeat(jnp.exp(heights), extent[dim] // blocks).reshape((-1,) + (1,) * (len(extent) - 1 - dim))
    return loudness


def noise(own_key, shape, scale, bound, split=(), dtype=jnp.bfloat16):
    result = jax.random.normal(own_key, shape, jnp.float32) * scale
    if len(split) > 0:
        result = shard_levels(own_key, shape, split, -0.22, 0.18) * result
    return jnp.clip(result, min=-bound, max=bound).astype(dtype)


def setup_inputs(seed: int = 0) -> dict:
    key_list = jax.random.split(jax.random.key(seed), 6)
    master = noise(key_list[0], (N_COL, D // 4, 4 * D // N_COL), 1.0, 6.0, ((0, 8), (1, 4)), jnp.float32)
    grad = noise(key_list[1], (N_COL, D // 4, 4 * D // N_COL), 1.0, 6.0, ((0, 8), (1, 4)))
    first_moment = noise(key_list[2], (N_COL, D // 4, 4 * D // N_COL), 1.0, 6.0, ((0, 8), (1, 4)), jnp.float32)
    second_moment = jnp.clip(jnp.exp(math.log(2.0) - 3.6888794 * jax.random.uniform(key_list[3], (N_COL, D // 4, 4 * D // N_COL), jnp.float32) ** shard_levels(key_list[3], (N_COL, D // 4, 4 * D // N_COL), ((0, 8), (1, 4)), -0.2, 0.2)), 0.05, 2.0)
    basis = noise(key_list[4], (N_COL, D // 4, 4 * D // N_COL), D ** -0.5, 0.0625, ((0, 8), (1, 4)))
    return dict(master=master, grad=grad, first_moment=first_moment, second_moment=second_moment, basis=basis)


def unpack(packed):
    width = D // N_COL
    return packed.reshape(N_COL, D // 4, 4, width).transpose(1, 2, 0, 3).reshape(D, D)

def pack(matrix):
    width = D // N_COL
    return matrix.reshape(D // 4, 4, N_COL, width).transpose(2, 0, 1, 3).reshape(N_COL, D // 4, 4 * width)

def reference(master, grad, first_moment, second_moment, basis):
    master = unpack(master)
    grad = unpack(grad)
    first_moment = unpack(first_moment)
    second_moment = unpack(second_moment)
    basis = unpack(basis)
    block = D // N_ROW
    grad_blocks = grad.reshape(N_ROW, block, D)
    basis_blocks = basis.reshape(N_ROW, block, D)

    def add_block(total, pair):
        grad_part, basis_part = pair
        term = lax.dot_general(basis_part, grad_part, (((0,), (0,)), ((), ())), preferred_element_type=jnp.float32)
        rounded = lax.optimization_barrier(term.astype(jnp.bfloat16))
        return (total + rounded.astype(jnp.float32), None)
    rotated, unused = lax.scan(add_block, jnp.zeros((D, D), jnp.float32), (grad_blocks, basis_blocks))
    new_first = 0.7 * first_moment + 0.3 * rotated
    new_second = 0.95 * second_moment + 0.05 * rotated * rotated
    direction = (new_first / (jnp.sqrt(new_second) + 1e-08)).astype(jnp.bfloat16)
    back = jnp.dot(basis, direction, preferred_element_type=jnp.float32)
    total = jnp.sum(back * back)
    factor = 1.0 / jnp.maximum(1.0, jnp.sqrt(total / (D * D)) / 0.5)
    new_master = master - 0.5 * factor * back
    return (pack(new_master), pack(new_master).astype(jnp.bfloat16), pack(new_first), pack(new_second))
```

```python
import functools

import jax
import jax.numpy as jnp
from jax import lax
from jax.experimental import pallas as pl
from jax.experimental.pallas import tpu as pltpu
from jax.sharding import PartitionSpec as P

VMEM_BYTES = 56 * 1024 * 1024


def cost(flops, moved):
    return pl.CostEstimate(flops=flops, bytes_accessed=moved, transcendentals=0)


def stack_quarters(block, width):
    return jnp.concatenate([block[:, q * width : (q + 1) * width] for q in range(4)], axis=0)


def rotate_kernel(width, basis_ref, grad_ref, out_ref):
    left = stack_quarters(basis_ref[...], width)
    right = stack_quarters(grad_ref[...], width)
    out_ref[...] = lax.dot_general(
        left, right, (((0,), (0,)), ((), ())), preferred_element_type=jnp.float32
    ).astype(out_ref.dtype)


def rotate(block, grad):
    groups, lanes = block.shape
    width = lanes // 4
    return pl.pallas_call(
        functools.partial(rotate_kernel, width),
        out_shape=jax.ShapeDtypeStruct((width, width), jnp.bfloat16),
        in_specs=[pl.BlockSpec(memory_space=pltpu.VMEM)] * 2,
        out_specs=pl.BlockSpec(memory_space=pltpu.VMEM),
        compiler_params=pltpu.CompilerParams(vmem_limit_bytes=VMEM_BYTES),
        cost_estimate=cost(8 * groups * width * width, 16 * groups * width + 2 * width * width),
    )(block, grad)


def adam_body(width, rot_ref, first_ref, second_ref, first_out, second_out, dir_out, rot, direction):
    rows = first_ref.shape[0]
    chunks = width // 128
    for u in range(chunks):
        rot[u] = rot_ref[:, u * 128 : (u + 1) * 128].astype(jnp.float32)
    for q in range(4):
        for u in range(chunks):
            part = slice(q * width + u * 128, q * width + (u + 1) * 128)
            rotated = rot[u, pl.ds(q, rows, stride=4), :]
            new_first = 0.7 * first_ref[:, part] + 0.3 * rotated
            new_second = 0.95 * second_ref[:, part] + 0.05 * rotated * rotated
            first_out[:, part] = new_first
            second_out[:, part] = new_second
            direction[u, pl.ds(q, rows, stride=4), :] = new_first / (jnp.sqrt(new_second) + 1e-08)
    for u in range(chunks):
        dir_out[:, u * 128 : (u + 1) * 128] = direction[u].astype(dir_out.dtype)


def adam(rotated, first, second):
    groups, lanes = first.shape
    width = lanes // 4
    tile = 64 if groups % 64 == 0 else groups
    row = pl.BlockSpec((tile, lanes), lambda i: (i, 0))
    flat = pl.BlockSpec((4 * tile, width), lambda i: (i, 0))
    return pl.pallas_call(
        functools.partial(adam_body, width),
        grid=(groups // tile,),
        in_specs=[flat, row, row],
        out_specs=[row, row, flat],
        out_shape=[
            jax.ShapeDtypeStruct(first.shape, jnp.float32),
            jax.ShapeDtypeStruct(first.shape, jnp.float32),
            jax.ShapeDtypeStruct((4 * groups, width), jnp.bfloat16),
        ],
        scratch_shapes=[pltpu.VMEM((width // 128, 4 * tile, 128), jnp.float32)] * 2,
        compiler_params=pltpu.CompilerParams(vmem_limit_bytes=VMEM_BYTES),
        cost_estimate=cost(20 * groups * lanes, 20 * groups * lanes),
    )(rotated, first, second)


def back_kernel(width, count, owner_ref, *refs):
    blocks, dir_ref, out_ref, sum_ref = refs[:count], refs[count], refs[count + 1], refs[count + 2]
    rows = out_ref.shape[0]
    total = None
    for s in range(count):
        left = stack_quarters(blocks[s][...], width)
        right = dir_ref[pl.ds(pl.multiple_of(owner_ref[s] * width, 128), width), :]
        term = jnp.dot(left, right, preferred_element_type=jnp.float32)
        total = term if total is None else total + term
    for q in range(4):
        out_ref[:, q * width : (q + 1) * width] = total[q * rows : (q + 1) * rows]
    sum_ref[...] = jnp.sum((total * total).reshape(-1, 8, width), axis=0)


def project(owners, blocks, direction):
    count = len(blocks)
    groups, lanes = blocks[0].shape
    width = lanes // 4
    tile = 112 if groups % 112 == 0 else groups
    row = pl.BlockSpec((tile, lanes), lambda i, owner: (i, 0))
    return pl.pallas_call(
        functools.partial(back_kernel, width, count),
        grid_spec=pltpu.PrefetchScalarGridSpec(
            num_scalar_prefetch=1,
            grid=(groups // tile,),
            in_specs=[row] * count + [pl.BlockSpec(memory_space=pltpu.VMEM)],
            out_specs=[row, pl.BlockSpec((8, width), lambda i, owner: (i, 0))],
        ),
        out_shape=[
            jax.ShapeDtypeStruct((groups, lanes), jnp.float32),
            jax.ShapeDtypeStruct((8 * (groups // tile), width), jnp.float32),
        ],
        compiler_params=pltpu.CompilerParams(vmem_limit_bytes=VMEM_BYTES),
        cost_estimate=cost(2 * count * groups * lanes * width, 2 * count * groups * lanes),
    )(owners, *blocks, direction)


def fast_body(n_row, n_col, master, grad, first_moment, second_moment, basis):
    groups, lanes = basis.shape[1:]
    width = lanes // 4
    size = width * n_col
    n_z = n_col // 2
    me = lax.axis_index("col")
    z, x = me // 2, me % 2
    up = [(i, (i + 2) % n_col) for i in range(n_col)]
    across = [(i, i ^ 1) for i in range(n_col)]

    grad = grad[0]
    blocks, owners, terms = [], [], []
    held, half = basis[0], groups // 2
    crossed = None
    for s in range(n_z):
        last = s == n_z - 1
        if last:
            parts = lax.ppermute(held[:half], "col", across), lax.ppermute(crossed[half:], "col", up)
            later, crossed = None, jnp.concatenate(parts, axis=0)
        else:
            later, crossed = lax.optimization_barrier(
                (lax.ppermute(held, "col", up), lax.ppermute(held, "col", across))
            )
        from_z = (z - s + n_z) % n_z
        for block, owner in ((held, 2 * from_z + x), (crossed, 2 * from_z + 1 - x)):
            blocks.append(block)
            owners.append(owner)
            terms.append(rotate(block, grad))
        held = later

    stacked = jnp.zeros((size, width), jnp.bfloat16)
    for owner, term in zip(owners, terms):
        stacked = lax.dynamic_update_slice(stacked, term, (owner * width, 0))
    rotated = lax.psum_scatter(stacked, "row", scatter_dimension=0, tiled=True)
    new_first, new_second, direction = adam(rotated, first_moment[0], second_moment[0])
    gathered = lax.all_gather(direction, "row", axis=0, tiled=True)
    back, squares = project(jnp.stack(owners).astype(jnp.int32), blocks, gathered)
    total = lax.psum(jnp.sum(squares), ("row", "col"))
    factor = 1.0 / jnp.maximum(1.0, jnp.sqrt(total / (size * size)) / 0.5)
    new_master = master - 0.5 * factor * back[None]
    return (new_master, new_master.astype(jnp.bfloat16), new_first[None], new_second[None])


def plain_body(master, grad, first_moment, second_moment, basis):
    width = grad.shape[2] // 4
    groups = grad.shape[1]
    quarter = width // 4
    grad_view = grad.reshape(groups, 4, width)
    panel = lax.all_gather(basis, "col", axis=0, tiled=True)
    blocks = panel.shape[0]
    size = blocks * width
    split = panel.reshape(blocks, groups, 4, width)
    term = jnp.einsum("cgqk,gqt->ckt", split, grad_view, preferred_element_type=jnp.float32)
    rotated = lax.psum_scatter(
        term.reshape(blocks * quarter, 4 * width).astype(jnp.bfloat16),
        "row",
        scatter_dimension=0,
        tiled=True,
    ).astype(jnp.float32)
    rotated = rotated.reshape(master.shape)
    new_first = 0.7 * first_moment + 0.3 * rotated
    new_second = 0.95 * second_moment + 0.05 * rotated * rotated
    direction = (new_first / (jnp.sqrt(new_second) + 1e-08)).astype(jnp.bfloat16)
    gathered = lax.all_gather(direction, "row", axis=1, tiled=True)
    stacked = gathered.reshape(blocks, width, width)
    back = jnp.einsum("cgqk,ckt->gqt", split, stacked, preferred_element_type=jnp.float32).reshape(
        master.shape
    )
    total = lax.psum(jnp.sum(back * back), ("row", "col"))
    factor = 1.0 / jnp.maximum(1.0, jnp.sqrt(total / (size * size)) / 0.5)
    new_master = master - 0.5 * factor * back
    return (new_master, new_master.astype(jnp.bfloat16), new_first, new_second)


def solution(mesh):
    n_row, n_col = mesh.shape["row"], mesh.shape["col"]

    def body(master, grad, first_moment, second_moment, basis):
        args = (master, grad, first_moment, second_moment, basis)
        if (grad.shape[2] // 4) % 128 == 0 and n_col == 2 * n_row:
            return fast_body(n_row, n_col, *args)
        return plain_body(*args)

    spec = P("col", "row", None)
    return jax.shard_map(
        body, mesh=mesh, in_specs=(spec,) * 5, out_specs=(spec,) * 4, check_vma=False
    )
```

```python
import functools

import jax
import jax.numpy as jnp
from jax import lax
from jax.experimental import pallas as pl
from jax.experimental.pallas import tpu as pltpu
from jax.sharding import PartitionSpec as P

VMEM_BYTES = 56 * 1024 * 1024


def cost(flops, moved):
    return pl.CostEstimate(flops=flops, bytes_accessed=moved, transcendentals=0)


def stack_quarters(block, width):
    return jnp.concatenate([block[:, q * width : (q + 1) * width] for q in range(4)], axis=0)


def rotate_kernel(width, basis_ref, grad_ref, out_ref):
    left = stack_quarters(basis_ref[...], width)
    right = stack_quarters(grad_ref[...], width)
    out_ref[...] = lax.dot_general(
        left, right, (((0,), (0,)), ((), ())), preferred_element_type=jnp.float32
    ).astype(out_ref.dtype)


def rotate(block, grad):
    groups, lanes = block.shape
    width = lanes // 4
    return pl.pallas_call(
        functools.partial(rotate_kernel, width),
        out_shape=jax.ShapeDtypeStruct((width, width), jnp.bfloat16),
        in_specs=[pl.BlockSpec(memory_space=pltpu.VMEM)] * 2,
        out_specs=pl.BlockSpec(memory_space=pltpu.VMEM),
        compiler_params=pltpu.CompilerParams(vmem_limit_bytes=VMEM_BYTES),
        cost_estimate=cost(8 * groups * width * width, 16 * groups * width + 2 * width * width),
    )(block, grad)


def adam_body(width, half_ref, rot_ref, first_ref, second_ref, *refs):
    first_out, second_out, dir_out, rot, direction = refs[-5:]
    rows = first_ref.shape[0]
    chunks = width // 128
    for u in range(chunks):
        rot[u] = rot_ref[:, u * 128 : (u + 1) * 128].astype(jnp.float32)
    for q in range(4):
        for u in range(chunks):
            part = slice(q * width + u * 128, q * width + (u + 1) * 128)
            rotated = rot[u, pl.ds(q, rows, stride=4), :]
            new_first = 0.7 * first_ref[:, part] + 0.3 * rotated
            new_second = 0.95 * second_ref[:, part] + 0.05 * rotated * rotated
            first_out[:, part] = new_first
            second_out[:, part] = new_second
            direction[u, pl.ds(q, rows, stride=4), :] = new_first / (jnp.sqrt(new_second) + 1e-08)
    for u in range(chunks):
        dir_out[:, u * 128 : (u + 1) * 128] = direction[u].astype(dir_out.dtype)


def adam(half, rotated, first, second, done=()):
    groups, lanes = first.shape
    width = lanes // 4
    rows = groups // 2
    tile = 56 if rows % 56 == 0 else rows
    steps = rows // tile
    row = pl.BlockSpec((tile, lanes), lambda i, half: (i + half[0] * steps, 0))
    flat = pl.BlockSpec((4 * tile, width), lambda i, half: (i, 0))
    return pl.pallas_call(
        functools.partial(adam_body, width),
        grid_spec=pltpu.PrefetchScalarGridSpec(
            num_scalar_prefetch=1,
            grid=(steps,),
            in_specs=[flat, row, row] + [pl.BlockSpec(memory_space=pl.ANY)] * len(done),
            out_specs=[row, row, flat],
            scratch_shapes=[pltpu.VMEM((width // 128, 4 * tile, 128), jnp.float32)] * 2,
        ),
        out_shape=[
            jax.ShapeDtypeStruct(first.shape, jnp.float32),
            jax.ShapeDtypeStruct(first.shape, jnp.float32),
            jax.ShapeDtypeStruct((4 * rows, width), jnp.bfloat16),
        ],
        input_output_aliases={4: 0, 5: 1} if done else {},
        compiler_params=pltpu.CompilerParams(vmem_limit_bytes=VMEM_BYTES),
        cost_estimate=cost(20 * rows * lanes, 20 * rows * lanes),
    )(half, rotated, first, second, *done)


def back_kernel(width, count, more, owner_ref, *refs):
    blocks, dir_ref, outs = refs[:count], refs[count], refs[count + 1 + more :]
    rows = outs[0].shape[0]
    total = None
    for s in range(count):
        left = stack_quarters(blocks[s][...], width)
        right = dir_ref[pl.ds(pl.multiple_of(owner_ref[s] * width, 128), width), :]
        term = jnp.dot(left, right, preferred_element_type=jnp.float32)
        total = term if total is None else total + term
    if more:
        total = total + stack_quarters(refs[count + 1][...], width)
    for q in range(4):
        outs[0][:, q * width : (q + 1) * width] = total[q * rows : (q + 1) * rows]
    if more:
        outs[1][...] = jnp.sum((total * total).reshape(-1, 8, width), axis=0)


def project(owners, blocks, direction, earlier=None):
    count = len(blocks)
    more = 0 if earlier is None else 1
    groups, lanes = blocks[0].shape
    width = lanes // 4
    tile = 112 if groups % 112 == 0 else groups
    row = pl.BlockSpec((tile, lanes), lambda i, owner: (i, 0))
    squares = pl.BlockSpec((8, width), lambda i, owner: (i, 0))
    out_shape = [
        jax.ShapeDtypeStruct((groups, lanes), jnp.float32),
        jax.ShapeDtypeStruct((8 * (groups // tile), width), jnp.float32),
    ]
    return pl.pallas_call(
        functools.partial(back_kernel, width, count, more),
        grid_spec=pltpu.PrefetchScalarGridSpec(
            num_scalar_prefetch=1,
            grid=(groups // tile,),
            in_specs=[row] * count + [pl.BlockSpec(memory_space=pltpu.VMEM)] + [row] * more,
            out_specs=[row, squares][: 1 + more],
        ),
        out_shape=out_shape[: 1 + more],
        compiler_params=pltpu.CompilerParams(vmem_limit_bytes=VMEM_BYTES),
        cost_estimate=cost(2 * count * groups * lanes * width, 2 * count * groups * lanes),
    )(owners, *blocks, direction, *([earlier] if more else []))


def spread_sum(value, n_row, n_col):
    held = jnp.full((8, 128), value, jnp.float32)
    turns = [("row", [[(i, (i + d) % n_row) for i in range(n_row)] for d in range(1, n_row)])]
    turns.append(
        ("col", [[(i, (i + 2 * d) % n_col) for i in range(n_col)] for d in range(1, n_col // 2)])
    )
    turns.append(("col", [[(i, i ^ 1) for i in range(n_col)]]))
    for axis, perms in turns:
        held = held + sum(lax.ppermute(held, axis, perm) for perm in perms)
    return held[0, 0]


def fast_body(n_row, n_col, master, grad, first_moment, second_moment, basis):
    groups, lanes = basis.shape[1:]
    width = lanes // 4
    size = width * n_col
    n_z = n_col // 2
    me = lax.axis_index("col")
    z, x = me // 2, me % 2
    up = [(i, (i + 2) % n_col) for i in range(n_col)]
    across = [(i, i ^ 1) for i in range(n_col)]

    grad = grad[0]
    blocks = []
    held, half = basis[0], groups // 2
    crossed = None
    for s in range(n_z):
        last = s == n_z - 1
        if last:
            first, second, held, blocks[-1] = lax.optimization_barrier(
                (held[:half], crossed[half:], held, blocks[-1])
            )
            parts = lax.ppermute(first, "col", across), lax.ppermute(second, "col", up)
            later, crossed = None, jnp.concatenate(parts, axis=0)
        else:
            later, crossed = lax.optimization_barrier(
                (lax.ppermute(held, "col", up), lax.ppermute(held, "col", across))
            )
        blocks += [held, crossed]
        held = later

    terms = [rotate(block, grad) for block in blocks]
    sides, done = (x, 1 - x), ()
    order = [(z - s + n_z) % n_z for s in range(n_z)]
    rotated = []
    for side in range(2):
        stacked = jnp.zeros((n_z * width, width), jnp.bfloat16)
        for s in range(n_z):
            stacked = lax.dynamic_update_slice(stacked, terms[2 * s + side], (order[s] * width, 0))
        rotated.append(lax.psum_scatter(stacked, "row", scatter_dimension=0, tiled=True))
    gathered = []
    for side in range(2):
        place = sides[side].astype(jnp.int32).reshape(1)
        *done, direction = adam(place, rotated[side], first_moment[0], second_moment[0], done)
        gathered.append(lax.all_gather(direction, "row", axis=0, tiled=True))
    new_first, new_second = done
    picks = jnp.stack(order).astype(jnp.int32)
    (back,) = project(picks, blocks[0::2], gathered[0])
    back, squares = project(picks, blocks[1::2], gathered[1], back)
    total = spread_sum(jnp.sum(squares), n_row, n_col)
    factor = 1.0 / jnp.maximum(1.0, jnp.sqrt(total / (size * size)) / 0.5)
    new_master = master - 0.5 * factor * back[None]
    return (new_master, new_master.astype(jnp.bfloat16), new_first[None], new_second[None])


def plain_body(master, grad, first_moment, second_moment, basis):
    width = grad.shape[2] // 4
    groups = grad.shape[1]
    quarter = width // 4
    grad_view = grad.reshape(groups, 4, width)
    panel = lax.all_gather(basis, "col", axis=0, tiled=True)
    blocks = panel.shape[0]
    size = blocks * width
    split = panel.reshape(blocks, groups, 4, width)
    term = jnp.einsum("cgqk,gqt->ckt", split, grad_view, preferred_element_type=jnp.float32)
    rotated = lax.psum_scatter(
        term.reshape(blocks * quarter, 4 * width).astype(jnp.bfloat16),
        "row",
        scatter_dimension=0,
        tiled=True,
    ).astype(jnp.float32)
    rotated = rotated.reshape(master.shape)
    new_first = 0.7 * first_moment + 0.3 * rotated
    new_second = 0.95 * second_moment + 0.05 * rotated * rotated
    direction = (new_first / (jnp.sqrt(new_second) + 1e-08)).astype(jnp.bfloat16)
    gathered = lax.all_gather(direction, "row", axis=1, tiled=True)
    stacked = gathered.reshape(blocks, width, width)
    back = jnp.einsum("cgqk,ckt->gqt", split, stacked, preferred_element_type=jnp.float32).reshape(
        master.shape
    )
    total = lax.psum(jnp.sum(back * back), ("row", "col"))
    factor = 1.0 / jnp.maximum(1.0, jnp.sqrt(total / (size * size)) / 0.5)
    new_master = master - 0.5 * factor * back
    return (new_master, new_master.astype(jnp.bfloat16), new_first, new_second)


def solution(mesh):
    n_row, n_col = mesh.shape["row"], mesh.shape["col"]

    def body(master, grad, first_moment, second_moment, basis):
        args = (master, grad, first_moment, second_moment, basis)
        if (grad.shape[2] // 4) % 128 == 0 and n_col == 2 * n_row:
            return fast_body(n_row, n_col, *args)
        return plain_body(*args)

    spec = P("col", "row", None)
    return jax.shard_map(
        body, mesh=mesh, in_specs=(spec,) * 5, out_specs=(spec,) * 4, check_vma=False
    )
```
